32 devices in a mesh: row: 4 (over x, core), col: 8 (over z, y).
Axes of the slice: x: 2, y: 2, z: 4, core: 2. Of those that a mesh axis runs over, the one named last changes fastest.
Arguments:
- rows: bfloat16 [1024, 4096], P(('row', 'col')), may hold values from -6 to 6
- task_ids: int32 [1024], P(('row', 'col')), may hold values from 0 to 8, as said below
- task_embed: bfloat16 [8, 4096], replicated, may hold values from -6 to 6
- norm_gain: float32 [4, 4096], replicated, may hold values from 0.1 to 1.9
- layer_weight: bfloat16 [4, 4096, 4096], P(None, None, 'col'), may hold values from -0.09375 to 0.09375
Outputs:
- packed_out: bfloat16 [1024, 4096], P('row', 'col')
The draws below stay inside these ranges and needn't reach their ends.
Inputs may be any that keep to these rules, and one draw needn't show every extreme that they name: `task_ids`: 8 marks an empty row, smaller values name a task.
All inputs are finite; a program needn't handle non-finite values.
Results may differ from the reference program's by a relative error of at most 0.008.
Values may be sent and summed in bfloat16 or wider, within the bound.
A program may use at most 128 MiB of HBM per device.

```python
import jax
import jax.numpy as jnp
from jax import lax

D = 4096
N_TASK = 8
LAYERS = 4
ROWS_DEV = 32
ROWS_TOTAL = 1024
N_ROW = 4
N_COL = 8


def draw_task_ids(key, part):
    first_key, second_key = jax.random.split(jax.random.fold_in(key, 11))
    device_count = N_ROW * N_COL
    live_rows = jax.random.randint(first_key, (device_count, 1), 3 * ROWS_DEV // 4, ROWS_DEV + 1)
    picked = jax.random.randint(second_key, (device_count, ROWS_DEV), 0, N_TASK)
    positions = jnp.arange(ROWS_DEV, dtype=jnp.int32)[None, :]
    table = jnp.where(positions < live_rows, picked, N_TASK)
    return table.reshape(-1).astype(jnp.int32)


def block_levels(rng, extent, cuts, least, largest):
    loudness = 1.0
    for position, blocks in cuts:
        draws = jax.random.uniform(jax.random.fold_in(jax.random.fold_in(rng, 6), position), (blocks,), jnp.float32, least / len(cuts), largest / len(cuts))
        loudness = loudness * jnp.repeat(jnp.exp(draws), extent[position] // blocks).reshape((-1,) + (1,) * (len(extent) - 1 - position))
    return loudness


def gaussian(key, extent, width, limit, shards=(), kind=jnp.bfloat16):
    drawn = jax.random.normal(key, extent, jnp.float32) * width
    if len(shards) > 0:
        drawn = block_levels(key, extent, shards, -0.22, 0.18) * drawn
    return jnp.clip(drawn, min=-limit, max=limit).astype(kind)


def setup_inputs(seed: int = 0) -> dict:
    streams_of = jax.random.split(jax.random.key(seed), 6)
    rows = gaussian(streams_of[0], (ROWS_TOTAL, D), 1.0, 6.0, ((0, 32),))
    task_ids = draw_task_ids(jax.random.fold_in(streams_of[5], 71), 0)
    task_embed = gaussian(streams_of[2], (N_TASK, D), 1.0, 6.0)
    norm_gain = jnp.clip(1.0 + 0.18 * jax.random.normal(streams_of[3], (LAYERS, D), jnp.float32), 0.1, 1.9)
    layer_weight = gaussian(streams_of[4], (LAYERS, D, D), D ** -0.5, 0.09375, ((2, 8),))
    return {"rows": rows, "task_ids": task_ids, "task_embed": task_embed, "norm_gain": norm_gain, "layer_weight": layer_weight}


epsilon = 1e-06

def reference(rows, task_ids, task_embed, norm_gain, layer_weight):
    device_count = N_ROW * N_COL
    row_total = device_count * ROWS_DEV
    task_table = task_ids.reshape(device_count, ROWS_DEV)
    task_range = jnp.arange(N_TASK, dtype=jnp.int32)
    member = (task_table[:, :, None] == task_range[None, None, :]).astype(jnp.int32)
    counts = lax.optimization_barrier(jnp.sum(member, axis=1)).astype(jnp.int32)
    before = (jnp.cumsum(counts, axis=0) - counts).astype(jnp.int32)
    totals = lax.optimization_barrier(jnp.sum(counts, axis=0)).astype(jnp.int32)
    task_base = (jnp.cumsum(totals) - totals).astype(jnp.int32)
    task_rank = lax.optimization_barrier(jnp.sum(member * (jnp.cumsum(member, axis=1) - member), axis=2)).astype(jnp.int32)
    packed_pos = (lax.optimization_barrier(jnp.sum(member * (task_base[None, None, :] + before[:, None, :]), axis=2)) + task_rank).astype(jnp.int32)
    target = jnp.where(task_table < N_TASK, packed_pos, row_total).reshape(-1).astype(jnp.int32)
    packed = jnp.zeros((row_total, D), jnp.bfloat16).at[target].set(rows, mode='drop')
    slot_pos = jnp.arange(row_total, dtype=jnp.int32)
    in_task = (slot_pos[:, None] >= task_base[None, :]) & (slot_pos[:, None] < (task_base + totals)[None, :])
    task_term = jnp.dot(in_task.astype(jnp.bfloat16), task_embed, preferred_element_type=jnp.float32)
    hidden = (packed.astype(jnp.float32) + task_term).astype(jnp.bfloat16)
    hidden = hidden.reshape(ROWS_DEV * N_COL, N_ROW, D).transpose(1, 0, 2).reshape(row_total, D)
    for layer_index in range(LAYERS):
        values = hidden.astype(jnp.float32)
        inverse_rms = lax.rsqrt(lax.optimization_barrier(jnp.mean(values * values, axis=1, keepdims=True)) + epsilon)
        active = jax.nn.silu(values * inverse_rms * norm_gain[layer_index][None, :]).astype(jnp.bfloat16)
        update = jnp.dot(active, layer_weight[layer_index], preferred_element_type=jnp.float32)
        hidden = (values + update).astype(jnp.bfloat16)
    return hidden
```

```python
import functools

import jax
import jax.numpy as jnp
from jax import lax
from jax.experimental import pallas as pl
from jax.experimental.pallas import tpu as pltpu
from jax.sharding import PartitionSpec as P

epsilon = 1e-06
MESH = pl.DeviceIdType.MESH
INNER = 2
CHUNKS = 4
LEAD = 1
F32 = jnp.float32
BF16 = jnp.bfloat16


def kernel(
    sizes,
    rows_ref,
    ids_ref,
    embed_ref,
    gain_ref,
    weight_ref,
    out_ref,
    weight,
    hidden,
    active,
    pieces,
    outgo,
    income,
    id_row,
    id_sum,
    id_col,
    sem_weight,
    sem_local,
    send_piece,
    recv_piece,
    send_idrow,
    recv_idrow,
    send_idcol,
    recv_idcol,
    send_row,
    recv_row,
    send_own,
    send_relay,
    recv_hidden,
):
    n_row, n_col, layers, chunks, tasks, cap = sizes
    n_outer = n_col // INNER
    rows_dev = rows_ref.shape[0]
    width = rows_ref.shape[1]
    part = width // n_col
    slots = rows_dev * n_col
    m = slots // chunks
    steps = layers * chunks
    me_r = lax.axis_index("row")
    me_c = lax.axis_index("col")
    outer = me_c // INNER
    inner = me_c % INNER
    partner = outer * INNER + (INNER - 1 - inner)

    def col_peer(j):
        return (me_c + j) % n_col

    def row_peer(j):
        return (me_r + j) % n_row

    def outer_peer(j):
        return ((outer + j) % n_outer) * INNER + inner

    def remote(src, dst, send, recv, r, c):
        return pltpu.make_async_remote_copy(
            src_ref=src, dst_ref=dst, send_sem=send, recv_sem=recv, device_id=(r, c), device_id_type=MESH
        )

    def weight_copy(l):
        return pltpu.make_async_copy(weight_ref.at[l], weight.at[l], sem_weight.at[l])

    barrier = pltpu.get_barrier_semaphore()
    for j in range(1, n_row):
        pl.semaphore_signal(barrier, inc=1, device_id=(row_peer(j), me_c), device_id_type=MESH)
    for j in range(1, n_col):
        pl.semaphore_signal(barrier, inc=1, device_id=(me_r, col_peer(j)), device_id_type=MESH)
    pl.semaphore_wait(barrier, n_row + n_col - 2)

    def id_row_copy(j):
        return remote(ids_ref, id_row.at[me_r], send_idrow.at[j], recv_idrow.at[me_r], row_peer(j), me_c)

    def id_row_from(j):
        return remote(ids_ref, id_row.at[row_peer(j)], send_idrow.at[j], recv_idrow.at[row_peer(j)], row_peer(j), me_c)

    def columns(c):
        return pl.ds(pl.multiple_of(c * part, part), part)

    def piece_copy(j):
        return remote(
            rows_ref.at[:, columns(col_peer(j))], pieces.at[me_c], send_piece.at[j], recv_piece.at[me_c], me_r, col_peer(j)
        )

    def piece_from(j):
        return remote(
            rows_ref.at[:, columns(col_peer(j))], pieces.at[col_peer(j)], send_piece.at[j], recv_piece.at[col_peer(j)],
            me_r, col_peer(j),
        )

    for j in range(1, n_row):
        id_row_copy(j).start()
    for j in range(1, n_col):
        piece_copy(j).start()
    for l in range(layers):
        weight_copy(l).start()
    pieces[me_c] = rows_ref[:, columns(me_c)]

    ids_here = ids_ref[...]
    for j in range(1, n_row):
        id_row_from(j).wait_recv()
        ids_here = ids_here + id_row[row_peer(j)]
    id_sum[...] = ids_here

    def id_col_copy(j):
        return remote(id_sum, id_col.at[me_c], send_idcol.at[j], recv_idcol.at[me_c], me_r, col_peer(j))

    def id_col_from(j):
        return remote(id_sum, id_col.at[col_peer(j)], send_idcol.at[j], recv_idcol.at[col_peer(j)], me_r, col_peer(j))

    for j in range(1, n_col):
        id_col_copy(j).start()
    low = lax.broadcasted_iota(jnp.int32, (slots, slots), 0)
    high = lax.broadcasted_iota(jnp.int32, (slots, slots), 1)
    earlier = jnp.where(low < high, 1.0, 0.0).astype(BF16)
    ids = ids_here
    for j in range(1, n_col):
        id_col_from(j).wait_recv()
        ids = ids + id_col[col_peer(j)]

    lead_dim = ids.shape[0]
    sub = lax.broadcasted_iota(jnp.int32, (lead_dim, slots), 0)
    sub_col = lax.broadcasted_iota(jnp.int32, (lead_dim, 1), 0)
    ids = jnp.where(sub < n_row, ids, tasks)
    live = ids < tasks
    member = [jnp.where(ids == t, 1.0, 0.0) for t in range(tasks)]
    ranks = jnp.dot(jnp.concatenate(member, 0).astype(BF16), earlier, preferred_element_type=F32)
    base = jnp.zeros((1, 1), F32)
    bases, ends = [], []
    position = jnp.zeros((lead_dim, slots), F32)
    for t in range(tasks):
        count = jnp.sum(member[t], axis=1, keepdims=True)
        bases.append(base)
        offset = jnp.zeros((lead_dim, 1), F32) + base
        for r in range(n_row):
            here = count[r : r + 1, :]
            offset = offset + jnp.where(sub_col > r, here, 0.0)
            base = base + here
        ends.append(base)
        rank = ranks[t * lead_dim : (t + 1) * lead_dim, :]
        position = position + member[t] * (offset + rank)
    slot = jnp.floor((position + 0.5) * (1.0 / n_row))
    target = jnp.where(live, position - slot * n_row, -1.0)
    aimed = [jnp.where(target == float(r), 1.0, 0.0) for r in range(n_row)]
    places = jnp.dot(jnp.concatenate(aimed, 0).astype(BF16), earlier, preferred_element_type=F32)
    place = jnp.zeros((lead_dim, slots), F32)
    for r in range(n_row):
        place = place + aimed[r] * places[r * lead_dim : (r + 1) * lead_dim, :]
    slot = slot.astype(jnp.int32)
    target = target.astype(jnp.int32)
    place = place.astype(jnp.int32)

    def of_me(values):
        picked = values[0:1, :]
        for r in range(1, n_row):
            picked = jnp.where(me_r == r, values[r : r + 1, :], picked)
        return picked

    cap_range = lax.broadcasted_iota(jnp.int32, (cap, slots), 0)

    def select(target_row, place_row, r):
        return jnp.where((cap_range == place_row) & (target_row == r), 1.0, 0.0).astype(BF16)

    my_target, my_place = of_me(target), of_me(place)
    picks = [select(my_target, my_place, row_peer(j)) for j in range(n_row)]
    slot_range = lax.broadcasted_iota(jnp.int32, (slots, slots), 0)

    for j in range(1, n_col):
        piece_from(j).wait_recv()
    group = pieces[...].reshape(slots, part)

    def row_copy(j):
        return remote(outgo.at[j], income.at[me_r], send_row.at[j], recv_row.at[me_r], row_peer(j), me_c)

    def row_from(j):
        return remote(outgo.at[j], income.at[row_peer(j)], send_row.at[j], recv_row.at[row_peer(j)], row_peer(j), me_c)

    for j in range(1, n_row):
        outgo[j] = jnp.dot(picks[j], group, preferred_element_type=F32).astype(BF16)
        row_copy(j).start()
    income[me_r] = jnp.dot(picks[0], group, preferred_element_type=F32).astype(BF16)

    puts = []
    for r in range(n_row):
        target_row = target[r : r + 1, :]
        here = jnp.where((slot_range == slot[r : r + 1, :]) & (target_row == me_r), 1.0, 0.0).astype(BF16)
        pick = select(target_row, place[r : r + 1, :], me_r)
        puts.append(
            lax.dot_general(here, pick, (((1,), (1,)), ((), ())), preferred_element_type=F32).astype(BF16)
        )
    slot_pos = (lax.broadcasted_iota(jnp.int32, (slots, 1), 0) * n_row + me_r).astype(F32)
    own_embed = embed_ref[:, columns(me_c)].astype(F32)
    start = jnp.zeros((slots, part), F32)
    for t in range(tasks):
        inside = jnp.where((slot_pos >= bases[t]) & (slot_pos < ends[t]), 1.0, 0.0)
        start = start + inside * own_embed[t : t + 1, :]
    for j in range(1, n_row):
        row_from(j).wait_recv()
    placed = jnp.zeros((slots, part), F32)
    for r in range(n_row):
        placed = placed + jnp.dot(puts[r], income[r], preferred_element_type=F32)
    start = (placed + start).astype(BF16)

    def own_copy(s, peer):
        mine = hidden.at[s, me_c]
        return remote(mine, mine, send_own.at[s % chunks, peer], recv_hidden.at[s, me_c], me_r, peer)

    def relay_copy(s, source):
        block = hidden.at[s, source]
        return remote(block, block, send_relay.at[s % chunks, source], recv_hidden.at[s, source], me_r, partner)

    def arrival(s, source):
        block = hidden.at[s, source]
        return remote(block, block, send_relay.at[s % chunks, source], recv_hidden.at[s, source], me_r, partner)

    def send_all(s):
        for j in range(1, n_outer):
            own_copy(s, outer_peer(j)).start()
        own_copy(s, partner).start()

    def drain_own(s):
        for j in range(1, n_outer):
            own_copy(s, outer_peer(j)).wait_send()
        own_copy(s, partner).wait_send()

    def relay_all(s):
        for j in range(1, n_outer):
            source = outer_peer(j)
            arrival(s, source).wait_recv()
            relay_copy(s, source).start()

    def drain_relay(s):
        for j in range(1, n_outer):
            relay_copy(s, outer_peer(j)).wait_send()

    for ch in range(chunks):
        hidden[ch, me_c] = start[ch * m : (ch + 1) * m, :]
        send_all(ch)
    for s in range(LEAD):
        relay_all(s)

    def step(s, carry):
        l = s // chunks
        ch = s % chunks
        ahead = s + LEAD

        @pl.when(ahead < steps)
        def _():
            @pl.when(ahead >= chunks)
            def _():
                drain_relay(ahead - chunks)

            relay_all(ahead)

        @pl.when(ch == 0)
        def _():
            weight_copy(l).wait()

        arrival(s, partner).wait_recv()
        for j in range(1, n_outer):
            source = ((outer + j) % n_outer) * INNER + (INNER - 1 - inner)
            arrival(s, source).wait_recv()

        total = jnp.zeros((m, part), F32)
        for c in range(n_col):
            values = hidden[s, c].astype(F32)
            total = total + values * values
        mean = jnp.sum(total, axis=1, keepdims=True) * (1.0 / width)
        inverse = lax.rsqrt(mean + epsilon)
        for c in range(n_col):
            cols = slice(c * part, (c + 1) * part)
            values = hidden[s, c].astype(F32) * inverse * gain_ref[l, :, cols]
            half = 0.5 * values
            active[:, cols] = (half + half * jnp.tanh(half)).astype(BF16)
        update = jnp.dot(active[...], weight[l], preferred_element_type=F32)
        result = (hidden[s, me_c].astype(F32) + update).astype(BF16)

        drain_own(s)

        @pl.when(l < layers - 1)
        def _():
            hidden[s + chunks, me_c] = result
            send_all(s + chunks)

        @pl.when(l == layers - 1)
        def _():
            out_ref[ch] = result

        return carry

    lax.fori_loop(0, steps, step, 0)

    for ch in range(chunks):
        drain_relay(steps - chunks + ch)
    for j in range(1, n_row):
        id_row_copy(j).wait_send()
        row_copy(j).wait_send()
    for j in range(1, n_col):
        piece_copy(j).wait_send()
        id_col_copy(j).wait_send()


def shards(rows, task_ids, task_embed, norm_gain, layer_weight):
    rows_dev, width = rows.shape
    tasks = task_embed.shape[0]
    layers = layer_weight.shape[0]
    part = layer_weight.shape[2]
    n_row = lax.axis_size("row")
    n_col = lax.axis_size("col")
    slots = rows_dev * n_col
    cap = -(-(slots // n_row + tasks) // 16) * 16
    chunks = CHUNKS
    m = slots // chunks
    lead_dim = -(-n_row // 8) * 8
    sub = lax.broadcasted_iota(jnp.int32, (lead_dim, slots), 0)
    lane = lax.broadcasted_iota(jnp.int32, (lead_dim, slots), 1)
    own = (sub == lax.axis_index("row")) & (lane // rows_dev == lax.axis_index("col"))
    ids = jnp.where(own, jnp.tile(task_ids, n_col)[None, :], 0)
    sizes = (n_row, n_col, layers, chunks, tasks, cap)
    dma = pltpu.SemaphoreType.DMA
    vmem = pl.BlockSpec(memory_space=pltpu.VMEM)
    out = pl.pallas_call(
        functools.partial(kernel, sizes),
        out_shape=jax.ShapeDtypeStruct((chunks, m, part), BF16),
        in_specs=[vmem, vmem, vmem, vmem, pl.BlockSpec(memory_space=pl.ANY)],
        out_specs=vmem,
        scratch_shapes=[
            pltpu.VMEM((layers, width, part), BF16),
            pltpu.VMEM((layers * chunks, n_col, m, part), BF16),
            pltpu.VMEM((m, width), BF16),
            pltpu.VMEM((n_col, rows_dev, part), BF16),
            pltpu.VMEM((n_row, cap, part), BF16),
            pltpu.VMEM((n_row, cap, part), BF16),
            pltpu.VMEM((n_row, lead_dim, slots), jnp.int32),
            pltpu.VMEM((lead_dim, slots), jnp.int32),
            pltpu.VMEM((n_col, lead_dim, slots), jnp.int32),
            dma((layers,)),
            dma,
            dma((n_col,)),
            dma((n_col,)),
            dma((n_row,)),
            dma((n_row,)),
            dma((n_col,)),
            dma((n_col,)),
            dma((n_row,)),
            dma((n_row,)),
            dma((chunks, n_col)),
            dma((chunks, n_col)),
            dma((layers * chunks, n_col)),
        ],
        compiler_params=pltpu.CompilerParams(
            collective_id=0, has_side_effects=True, vmem_limit_bytes=60 * 1024 * 1024
        ),
    )(rows, ids, task_embed, norm_gain.reshape(layers, 1, width), layer_weight)
    return out.reshape(slots, part)


def solution(mesh):
    return jax.shard_map(
        shards,
        mesh=mesh,
        in_specs=(P(("row", "col"), None), P(("row", "col")), P(), P(), P(None, None, "col")),
        out_specs=P("row", "col"),
        check_vma=False,
    )
```

```python
import functools

import jax
import jax.numpy as jnp
from jax import lax
from jax.experimental import pallas as pl
from jax.experimental.pallas import tpu as pltpu
from jax.sharding import PartitionSpec as P

epsilon = 1e-06
MESH = pl.DeviceIdType.MESH
INNER = 2
CHUNKS = 4
LEAD1 = 2
LEAD2 = 1
F32 = jnp.float32
BF16 = jnp.bfloat16


def kernel(
    sizes,
    rows_ref,
    ids_ref,
    embed_ref,
    gain_ref,
    weight_ref,
    out_ref,
    weight,
    hidden,
    active,
    gain,
    pieces,
    outgo,
    income,
    id_own,
    id_row,
    id_sum,
    id_col,
    sem_weight,
    send_piece,
    recv_piece,
    send_idrow,
    recv_idrow,
    send_idcol,
    recv_idcol,
    send_row,
    recv_row,
    send_own,
    send_relay,
    send_along,
    recv_hidden,
):
    n_row, n_col, layers, chunks, tasks, cap = sizes
    n_outer = n_col // INNER
    rows_dev = rows_ref.shape[0]
    width = rows_ref.shape[1]
    part = width // n_col
    slots = rows_dev * n_col
    m = slots // chunks
    steps = layers * chunks
    me_r = lax.axis_index("row")
    me_c = lax.axis_index("col")
    outer = me_c // INNER
    inner = me_c % INNER
    partner = outer * INNER + (INNER - 1 - inner)

    def col_peer(j):
        return (me_c + j) % n_col

    def row_peer(j):
        return (me_r + j) % n_row

    def outer_peer(j):
        return ((outer + j) % n_outer) * INNER + inner

    def remote(src, dst, send, recv, r, c):
        return pltpu.make_async_remote_copy(
            src_ref=src, dst_ref=dst, send_sem=send, recv_sem=recv, device_id=(r, c), device_id_type=MESH
        )

    def weight_copy(l):
        return pltpu.make_async_copy(weight_ref.at[l], weight.at[l], sem_weight.at[l])

    lead_dim = id_own.shape[0]
    spread = lax.broadcasted_iota(jnp.int32, (rows_dev, slots), 1) - lax.broadcasted_iota(
        jnp.int32, (rows_dev, slots), 0
    )
    spread = jnp.where(spread == me_c * rows_dev, 1.0, 0.0).astype(BF16)
    own_ids = jnp.broadcast_to(ids_ref[...].astype(F32), (lead_dim, rows_dev)).astype(BF16)
    own_ids = jnp.dot(own_ids, spread, preferred_element_type=F32).astype(jnp.int32)
    sub = lax.broadcasted_iota(jnp.int32, (lead_dim, slots), 0)
    id_own[...] = jnp.where(sub == me_r, own_ids, 0)

    barrier = pltpu.get_barrier_semaphore()
    for j in range(1, n_row):
        pl.semaphore_signal(barrier, inc=1, device_id=(row_peer(j), me_c), device_id_type=MESH)
    for j in range(1, n_col):
        pl.semaphore_signal(barrier, inc=1, device_id=(me_r, col_peer(j)), device_id_type=MESH)
    pl.semaphore_wait(barrier, n_row + n_col - 2)

    def id_row_copy(j):
        return remote(id_own, id_row.at[me_r], send_idrow.at[j], recv_idrow.at[me_r], row_peer(j), me_c)

    def id_row_from(j):
        return remote(id_own, id_row.at[row_peer(j)], send_idrow.at[j], recv_idrow.at[row_peer(j)], row_peer(j), me_c)

    def columns(c):
        return pl.ds(pl.multiple_of(c * part, part), part)

    def piece_copy(j):
        return remote(
            rows_ref.at[:, columns(col_peer(j))], pieces.at[me_c], send_piece.at[j], recv_piece.at[me_c], me_r, col_peer(j)
        )

    def piece_from(j):
        return remote(
            rows_ref.at[:, columns(col_peer(j))], pieces.at[col_peer(j)], send_piece.at[j], recv_piece.at[col_peer(j)],
            me_r, col_peer(j),
        )

    for j in range(1, n_row):
        id_row_copy(j).start()
    for j in range(1, n_col):
        piece_copy(j).start()
    for l in range(layers):
        weight_copy(l).start()
    pieces[me_c] = rows_ref[:, columns(me_c)]
    for l in range(layers):
        gain[l] = gain_ref[l : l + 1, :]

    ids_here = id_own[...]
    for j in range(1, n_row):
        id_row_from(j).wait_recv()
        ids_here = ids_here + id_row[row_peer(j)]
    id_sum[...] = ids_here

    def id_col_copy(j):
        return remote(id_sum, id_col.at[me_c], send_idcol.at[j], recv_idcol.at[me_c], me_r, col_peer(j))

    def id_col_from(j):
        return remote(id_sum, id_col.at[col_peer(j)], send_idcol.at[j], recv_idcol.at[col_peer(j)], me_r, col_peer(j))

    for j in range(1, n_col):
        id_col_copy(j).start()
    low = lax.broadcasted_iota(jnp.int32, (slots, slots), 0)
    high = lax.broadcasted_iota(jnp.int32, (slots, slots), 1)
    earlier = jnp.where(low < high, 1.0, 0.0).astype(BF16)
    ids = ids_here
    for j in range(1, n_col):
        id_col_from(j).wait_recv()
        ids = ids + id_col[col_peer(j)]

    sub_col = lax.broadcasted_iota(jnp.int32, (lead_dim, 1), 0)
    ids = jnp.where(sub < n_row, ids, tasks)
    live = ids < tasks
    member = [jnp.where(ids == t, 1.0, 0.0) for t in range(tasks)]
    ranks = jnp.dot(jnp.concatenate(member, 0).astype(BF16), earlier, preferred_element_type=F32)
    base = jnp.zeros((1, 1), F32)
    bases, ends = [], []
    position = jnp.zeros((lead_dim, slots), F32)
    for t in range(tasks):
        count = jnp.sum(member[t], axis=1, keepdims=True)
        bases.append(base)
        offset = jnp.zeros((lead_dim, 1), F32) + base
        for r in range(n_row):
            here = count[r : r + 1, :]
            offset = offset + jnp.where(sub_col > r, here, 0.0)
            base = base + here
        ends.append(base)
        rank = ranks[t * lead_dim : (t + 1) * lead_dim, :]
        position = position + member[t] * (offset + rank)
    slot = jnp.floor((position + 0.5) * (1.0 / n_row))
    target = jnp.where(live, position - slot * n_row, -1.0)
    aimed = [jnp.where(target == float(r), 1.0, 0.0) for r in range(n_row)]
    places = jnp.dot(jnp.concatenate(aimed, 0).astype(BF16), earlier, preferred_element_type=F32)
    place = jnp.zeros((lead_dim, slots), F32)
    for r in range(n_row):
        place = place + aimed[r] * places[r * lead_dim : (r + 1) * lead_dim, :]
    slot = slot.astype(jnp.int32)
    target = target.astype(jnp.int32)
    place = place.astype(jnp.int32)

    def of_me(values):
        picked = values[0:1, :]
        for r in range(1, n_row):
            picked = jnp.where(me_r == r, values[r : r + 1, :], picked)
        return picked

    cap_range = lax.broadcasted_iota(jnp.int32, (cap, slots), 0)

    def select(target_row, place_row, r):
        return jnp.where((cap_range == place_row) & (target_row == r), 1.0, 0.0).astype(BF16)

    my_target, my_place = of_me(target), of_me(place)
    picks = [select(my_target, my_place, row_peer(j)) for j in range(n_row)]
    slot_range = lax.broadcasted_iota(jnp.int32, (slots, slots), 0)

    for j in range(1, n_col):
        piece_from(j).wait_recv()
    group = pieces[...].reshape(slots, part)

    def row_copy(j):
        return remote(outgo.at[j], income.at[me_r], send_row.at[j], recv_row.at[me_r], row_peer(j), me_c)

    def row_from(j):
        return remote(outgo.at[j], income.at[row_peer(j)], send_row.at[j], recv_row.at[row_peer(j)], row_peer(j), me_c)

    for j in range(1, n_row):
        outgo[j] = jnp.dot(picks[j], group, preferred_element_type=F32).astype(BF16)
        row_copy(j).start()
    income[me_r] = jnp.dot(picks[0], group, preferred_element_type=F32).astype(BF16)

    puts = []
    for r in range(n_row):
        target_row = target[r : r + 1, :]
        here = jnp.where((slot_range == slot[r : r + 1, :]) & (target_row == me_r), 1.0, 0.0).astype(BF16)
        pick = select(target_row, place[r : r + 1, :], me_r)
        puts.append(
            lax.dot_general(here, pick, (((1,), (1,)), ((), ())), preferred_element_type=F32).astype(BF16)
        )
    slot_pos = (lax.broadcasted_iota(jnp.int32, (slots, 1), 0) * n_row + me_r).astype(F32)
    own_embed = embed_ref[:, columns(me_c)].astype(F32)
    start = jnp.zeros((slots, part), F32)
    for t in range(tasks):
        inside = jnp.where((slot_pos >= bases[t]) & (slot_pos < ends[t]), 1.0, 0.0)
        start = start + inside * own_embed[t : t + 1, :]
    for j in range(1, n_row):
        row_from(j).wait_recv()
    placed = jnp.zeros((slots, part), F32)
    for r in range(n_row):
        placed = placed + jnp.dot(puts[r], income[r], preferred_element_type=F32)
    start = (placed + start).astype(BF16)

    half = n_outer // 2
    side = outer // half
    is_gate = outer == half - 1 + side
    far_gate = (half - side) * INNER + inner

    def near(j, i):
        return (side * half + (outer % half + j) % half) * INNER + i

    def far(k, i):
        return ((1 - side) * half + k) * INNER + i

    other = INNER - 1 - inner

    def block_copy(s, source, send, peer):
        block = hidden.at[s, source]
        return remote(block, block, send, recv_hidden.at[s, source], me_r, peer)

    def await_block(s, source):
        block_copy(s, source, send_relay.at[0, source], partner).wait_recv()

    def own_copies(s):
        peers = [near(j, inner) for j in range(1, half)] + [far_gate, partner]
        return [block_copy(s, me_c, send_own.at[s % chunks, peer], peer) for peer in peers]

    def send_all(s):
        for copy in own_copies(s):
            copy.start()

    def drain_own(s):
        for copy in own_copies(s):
            copy.wait_send()

    def over(s, source):
        return block_copy(s, source, send_relay.at[s % chunks, source], partner)

    def along(s, source, j):
        return block_copy(s, source, send_along.at[s % chunks, source // INNER, j], near(j, inner))

    def pass_on(s, go, source, copies):
        if go:
            await_block(s, source)
        for copy in copies:
            if go:
                copy.start()
            else:
                copy.wait_send()

    def first_relay(s, go):
        @pl.when(is_gate)
        def _():
            for k in range(half):
                source = far(k, inner)
                pass_on(s, go, source, [along(s, source, j) for j in range(1, half)] + [over(s, source)])

        @pl.when(s % 2 == 0)
        def _():
            for j in range(1, half):
                pass_on(s, go, near(j, inner), [over(s, near(j, inner))])

        @pl.when(s % 2 == 1)
        def _():
            pass_on(s, go, partner, [along(s, partner, j) for j in range(1, half)])

    def second_relay(s, go):
        @pl.when(jnp.logical_not(is_gate))
        def _():
            for k in range(half):
                pass_on(s, go, far(k, inner), [over(s, far(k, inner))])

    def await_rest(s):
        @pl.when(s % 2 == 0)
        def _():
            await_block(s, partner)

        @pl.when(s % 2 == 1)
        def _():
            for j in range(1, half):
                await_block(s, near(j, inner))

        for j in range(1, half):
            await_block(s, near(j, other))
        for k in range(half):
            await_block(s, far(k, other))

    def relay(s, relay_of):
        @pl.when(s < steps)
        def _():
            @pl.when(s >= chunks)
            def _():
                relay_of(s - chunks, False)

            relay_of(s, True)

    for ch in range(chunks):
        hidden[ch, me_c] = start[ch * m : (ch + 1) * m, :]
        send_all(ch)
    for s in range(LEAD1):
        first_relay(jnp.int32(s), True)
    for s in range(LEAD2):
        second_relay(jnp.int32(s), True)

    def step(s, carry):
        l = s // chunks
        ch = s % chunks
        relay(s + LEAD2, second_relay)
        relay(s + LEAD1, first_relay)

        @pl.when(ch == 0)
        def _():
            weight_copy(l).wait()

        await_rest(s)
        total = jnp.zeros((m, part), F32)
        for c in range(n_col):
            values = hidden[s, c].astype(F32)
            total = total + values * values
        mean = jnp.sum(total, axis=1, keepdims=True) * (1.0 / width)
        inverse = lax.rsqrt(mean + epsilon)
        for c in range(n_col):
            cols = slice(c * part, (c + 1) * part)
            values = hidden[s, c].astype(F32) * inverse * gain[l, :, cols]
            half = 0.5 * values
            active[:, cols] = (half + half * jnp.tanh(half)).astype(BF16)
        update = jnp.dot(active[...], weight[l], preferred_element_type=F32)
        result = (hidden[s, me_c].astype(F32) + update).astype(BF16)

        drain_own(s)

        @pl.when(l < layers - 1)
        def _():
            hidden[s + chunks, me_c] = result
            send_all(s + chunks)

        @pl.when(l == layers - 1)
        def _():
            out_ref[ch] = result

        return carry

    lax.fori_loop(0, steps, step, 0)

    for ch in range(chunks):
        first_relay(jnp.int32(steps - chunks + ch), False)
        second_relay(jnp.int32(steps - chunks + ch), False)
    for j in range(1, n_row):
        id_row_copy(j).wait_send()
        row_copy(j).wait_send()
    for j in range(1, n_col):
        piece_copy(j).wait_send()
        id_col_copy(j).wait_send()


def shards(rows, task_ids, task_embed, norm_gain, layer_weight):
    rows_dev, width = rows.shape
    tasks = task_embed.shape[0]
    layers = layer_weight.shape[0]
    part = layer_weight.shape[2]
    n_row = lax.axis_size("row")
    n_col = lax.axis_size("col")
    slots = rows_dev * n_col
    cap = -(-(slots // n_row + tasks) // 16) * 16
    chunks = CHUNKS
    m = slots // chunks
    lead_dim = -(-n_row // 8) * 8
    sizes = (n_row, n_col, layers, chunks, tasks, cap)
    dma = pltpu.SemaphoreType.DMA
    vmem = pl.BlockSpec(memory_space=pltpu.VMEM)
    out = pl.pallas_call(
        functools.partial(kernel, sizes),
        out_shape=jax.ShapeDtypeStruct((chunks, m, part), BF16),
        in_specs=[vmem, vmem, vmem, vmem, pl.BlockSpec(memory_space=pl.ANY)],
        out_specs=vmem,
        scratch_shapes=[
            pltpu.VMEM((layers, width, part), BF16),
            pltpu.VMEM((layers * chunks, n_col, m, part), BF16),
            pltpu.VMEM((m, width), BF16),
            pltpu.VMEM((layers, 1, width), F32),
            pltpu.VMEM((n_col, rows_dev, part), BF16),
            pltpu.VMEM((n_row, cap, part), BF16),
            pltpu.VMEM((n_row, cap, part), BF16),
            pltpu.VMEM((lead_dim, slots), jnp.int32),
            pltpu.VMEM((n_row, lead_dim, slots), jnp.int32),
            pltpu.VMEM((lead_dim, slots), jnp.int32),
            pltpu.VMEM((n_col, lead_dim, slots), jnp.int32),
            dma((layers,)),
            dma((n_col,)),
            dma((n_col,)),
            dma((n_row,)),
            dma((n_row,)),
            dma((n_col,)),
            dma((n_col,)),
            dma((n_row,)),
            dma((n_row,)),
            dma((chunks, n_col)),
            dma((chunks, n_col)),
            dma((chunks, n_col // INNER, max(1, n_col // INNER // 2))),
            dma((layers * chunks, n_col)),
        ],
        compiler_params=pltpu.CompilerParams(
            collective_id=0, has_side_effects=True, vmem_limit_bytes=60 * 1024 * 1024
        ),
    )(rows, task_ids.reshape(1, rows_dev), task_embed, norm_gain, layer_weight)
    return out.reshape(slots, part)


def solution(mesh):
    return jax.shard_map(
        shards,
        mesh=mesh,
        in_specs=(P(("row", "col"), None), P(("row", "col")), P(), P(), P(None, None, "col")),
        out_specs=P("row", "col"),
        check_vma=False,
    )
```

```python
import functools

import jax
import jax.numpy as jnp
from jax import lax
from jax.experimental import pallas as pl
from jax.experimental.pallas import tpu as pltpu
from jax.sharding import PartitionSpec as P

epsilon = 1e-06
MESH = pl.DeviceIdType.MESH
INNER = 2
CHUNKS = 4
LEAD1 = 2
LEAD2 = 1
F32 = jnp.float32
BF16 = jnp.bfloat16


def kernel(
    sizes,
    rows_ref,
    ids_ref,
    embed_ref,
    gain_ref,
    weight_ref,
    out_ref,
    weight,
    hidden,
    active,
    gain,
    pieces,
    outgo,
    income,
    id_own,
    id_row,
    id_sum,
    id_col,
    sem_weight,
    send_piece,
    recv_piece,
    send_idrow,
    recv_idrow,
    send_idcol,
    recv_idcol,
    send_row,
    recv_row,
    send_own,
    send_relay,
    send_along,
    recv_hidden,
):
    n_row, n_col, layers, chunks, tasks, cap = sizes
    n_outer = n_col // INNER
    rows_dev = rows_ref.shape[0]
    width = rows_ref.shape[1]
    part = width // n_col
    slots = rows_dev * n_col
    m = slots // chunks
    steps = layers * chunks
    me_r = lax.axis_index("row")
    me_c = lax.axis_index("col")
    outer = me_c // INNER
    inner = me_c % INNER
    partner = outer * INNER + (INNER - 1 - inner)

    def col_peer(j):
        return (me_c + j) % n_col

    def row_peer(j):
        return (me_r + j) % n_row

    def outer_peer(j):
        return ((outer + j) % n_outer) * INNER + inner

    def remote(src, dst, send, recv, r, c):
        return pltpu.make_async_remote_copy(
            src_ref=src, dst_ref=dst, send_sem=send, recv_sem=recv, device_id=(r, c), device_id_type=MESH
        )

    def weight_copy(l):
        return pltpu.make_async_copy(weight_ref.at[l], weight.at[l], sem_weight.at[l])

    lead_dim = id_own.shape[0]
    spread = lax.broadcasted_iota(jnp.int32, (rows_dev, slots), 1) - lax.broadcasted_iota(
        jnp.int32, (rows_dev, slots), 0
    )
    spread = jnp.where(spread == me_c * rows_dev, 1.0, 0.0).astype(BF16)
    own_ids = jnp.broadcast_to(ids_ref[...].astype(F32), (lead_dim, rows_dev)).astype(BF16)
    own_ids = jnp.dot(own_ids, spread, preferred_element_type=F32).astype(jnp.int32)
    sub = lax.broadcasted_iota(jnp.int32, (lead_dim, slots), 0)
    id_own[...] = jnp.where(sub == me_r, own_ids, 0)

    barrier = pltpu.get_barrier_semaphore()
    for j in range(1, n_row):
        pl.semaphore_signal(barrier, inc=1, device_id=(row_peer(j), me_c), device_id_type=MESH)
    for j in range(1, n_col):
        pl.semaphore_signal(barrier, inc=1, device_id=(me_r, col_peer(j)), device_id_type=MESH)
    pl.semaphore_wait(barrier, n_row + n_col - 2)

    def id_row_copy(j):
        return remote(id_own, id_row.at[me_r], send_idrow.at[j], recv_idrow.at[me_r], row_peer(j), me_c)

    def id_row_from(j):
        return remote(id_own, id_row.at[row_peer(j)], send_idrow.at[j], recv_idrow.at[row_peer(j)], row_peer(j), me_c)

    def columns(c):
        return pl.ds(pl.multiple_of(c * part, part), part)

    def piece_copy(j):
        return remote(
            rows_ref.at[:, columns(col_peer(j))], pieces.at[me_c], send_piece.at[j], recv_piece.at[me_c], me_r, col_peer(j)
        )

    def piece_from(j):
        return remote(
            rows_ref.at[:, columns(col_peer(j))], pieces.at[col_peer(j)], send_piece.at[j], recv_piece.at[col_peer(j)],
            me_r, col_peer(j),
        )

    for j in range(1, n_row):
        id_row_copy(j).start()
    for j in range(1, n_col):
        piece_copy(j).start()
    for l in range(layers):
        weight_copy(l).start()
    pieces[me_c] = rows_ref[:, columns(me_c)]
    for l in range(layers):
        gain[l] = gain_ref[l : l + 1, :]

    ids_here = id_own[...]
    for j in range(1, n_row):
        id_row_from(j).wait_recv()
        ids_here = ids_here + id_row[row_peer(j)]
    id_sum[...] = ids_here

    def id_col_copy(j):
        return remote(id_sum, id_col.at[me_c], send_idcol.at[j], recv_idcol.at[me_c], me_r, col_peer(j))

    def id_col_from(j):
        return remote(id_sum, id_col.at[col_peer(j)], send_idcol.at[j], recv_idcol.at[col_peer(j)], me_r, col_peer(j))

    for j in range(1, n_col):
        id_col_copy(j).start()
    low = lax.broadcasted_iota(jnp.int32, (slots, slots), 0)
    high = lax.broadcasted_iota(jnp.int32, (slots, slots), 1)
    earlier = jnp.where(low < high, 1.0, 0.0).astype(BF16)
    ids = ids_here
    for j in range(1, n_col):
        id_col_from(j).wait_recv()
        ids = ids + id_col[col_peer(j)]

    sub_col = lax.broadcasted_iota(jnp.int32, (lead_dim, 1), 0)
    ids = jnp.where(sub < n_row, ids, tasks)
    live = ids < tasks
    member = [jnp.where(ids == t, 1.0, 0.0) for t in range(tasks)]
    ranks = jnp.dot(jnp.concatenate(member, 0).astype(BF16), earlier, preferred_element_type=F32)
    base = jnp.zeros((1, 1), F32)
    bases, ends = [], []
    position = jnp.zeros((lead_dim, slots), F32)
    for t in range(tasks):
        count = jnp.sum(member[t], axis=1, keepdims=True)
        bases.append(base)
        offset = jnp.zeros((lead_dim, 1), F32) + base
        for r in range(n_row):
            here = count[r : r + 1, :]
            offset = offset + jnp.where(sub_col > r, here, 0.0)
            base = base + here
        ends.append(base)
        rank = ranks[t * lead_dim : (t + 1) * lead_dim, :]
        position = position + member[t] * (offset + rank)
    slot = jnp.floor((position + 0.5) * (1.0 / n_row))
    target = jnp.where(live, position - slot * n_row, -1.0)
    aimed = [jnp.where(target == float(r), 1.0, 0.0) for r in range(n_row)]
    places = jnp.dot(jnp.concatenate(aimed, 0).astype(BF16), earlier, preferred_element_type=F32)
    place = jnp.zeros((lead_dim, slots), F32)
    for r in range(n_row):
        place = place + aimed[r] * places[r * lead_dim : (r + 1) * lead_dim, :]
    slot = slot.astype(jnp.int32)
    target = target.astype(jnp.int32)
    place = place.astype(jnp.int32)

    def of_me(values):
        picked = values[0:1, :]
        for r in range(1, n_row):
            picked = jnp.where(me_r == r, values[r : r + 1, :], picked)
        return picked

    cap_range = lax.broadcasted_iota(jnp.int32, (cap, slots), 0)

    def select(target_row, place_row, r):
        return jnp.where((cap_range == place_row) & (target_row == r), 1.0, 0.0).astype(BF16)

    my_target, my_place = of_me(target), of_me(place)
    picks = [select(my_target, my_place, row_peer(j)) for j in range(n_row)]
    slot_range = lax.broadcasted_iota(jnp.int32, (slots, slots), 0)

    for j in range(1, n_col):
        piece_from(j).wait_recv()
    group = pieces[...].reshape(slots, part)

    def row_copy(j):
        return remote(outgo.at[j], income.at[me_r], send_row.at[j], recv_row.at[me_r], row_peer(j), me_c)

    def row_from(j):
        return remote(outgo.at[j], income.at[row_peer(j)], send_row.at[j], recv_row.at[row_peer(j)], row_peer(j), me_c)

    for j in range(1, n_row):
        outgo[j] = jnp.dot(picks[j], group, preferred_element_type=F32).astype(BF16)
        row_copy(j).start()
    income[me_r] = jnp.dot(picks[0], group, preferred_element_type=F32).astype(BF16)

    puts = []
    for r in range(n_row):
        target_row = target[r : r + 1, :]
        here = jnp.where((slot_range == slot[r : r + 1, :]) & (target_row == me_r), 1.0, 0.0).astype(BF16)
        pick = select(target_row, place[r : r + 1, :], me_r)
        puts.append(
            lax.dot_general(here, pick, (((1,), (1,)), ((), ())), preferred_element_type=F32).astype(BF16)
        )
    slot_pos = (lax.broadcasted_iota(jnp.int32, (slots, 1), 0) * n_row + me_r).astype(F32)
    own_embed = embed_ref[:, columns(me_c)].astype(F32)
    start = jnp.zeros((slots, part), F32)
    for t in range(tasks):
        inside = jnp.where((slot_pos >= bases[t]) & (slot_pos < ends[t]), 1.0, 0.0)
        start = start + inside * own_embed[t : t + 1, :]
    for j in range(1, n_row):
        row_from(j).wait_recv()

    half = n_outer // 2
    side = outer // half
    is_gate = outer == half - 1 + side
    far_gate = (half - side) * INNER + inner

    def near(j, i):
        return (side * half + (outer % half + j) % half) * INNER + i

    def far(k, i):
        return ((1 - side) * half + k) * INNER + i

    other = INNER - 1 - inner

    def block_copy(s, source, send, peer):
        block = hidden.at[s, source]
        return remote(block, block, send, recv_hidden.at[s, source], me_r, peer)

    def await_block(s, source):
        block_copy(s, source, send_relay.at[0, source], partner).wait_recv()

    def own_copies(s):
        peers = [near(j, inner) for j in range(1, half)] + [far_gate, partner]
        return [block_copy(s, me_c, send_own.at[s % chunks, peer], peer) for peer in peers]

    def send_all(s):
        for copy in own_copies(s):
            copy.start()

    def drain_own(s):
        for copy in own_copies(s):
            copy.wait_send()

    def over(s, source):
        return block_copy(s, source, send_relay.at[s % chunks, source], partner)

    def along(s, source, j):
        return block_copy(s, source, send_along.at[s % chunks, source // INNER, j], near(j, inner))

    def pass_on(s, go, source, copies):
        if go:
            await_block(s, source)
        for copy in copies:
            if go:
                copy.start()
            else:
                copy.wait_send()

    def first_relay(s, go):
        @pl.when(is_gate)
        def _():
            for k in range(half):
                source = far(k, inner)
                pass_on(s, go, source, [along(s, source, j) for j in range(1, half)] + [over(s, source)])

        @pl.when(s % 2 == 0)
        def _():
            for j in range(1, half):
                pass_on(s, go, near(j, inner), [over(s, near(j, inner))])

        @pl.when(s % 2 == 1)
        def _():
            pass_on(s, go, partner, [along(s, partner, j) for j in range(1, half)])

    def second_relay(s, go):
        @pl.when(jnp.logical_not(is_gate))
        def _():
            for k in range(half):
                pass_on(s, go, far(k, inner), [over(s, far(k, inner))])

    def await_rest(s):
        @pl.when(s % 2 == 0)
        def _():
            await_block(s, partner)

        @pl.when(s % 2 == 1)
        def _():
            for j in range(1, half):
                await_block(s, near(j, inner))

        for j in range(1, half):
            await_block(s, near(j, other))
        for k in range(half):
            await_block(s, far(k, other))

    def relay(s, relay_of):
        @pl.when(s < steps)
        def _():
            @pl.when(s >= chunks)
            def _():
                relay_of(s - chunks, False)

            relay_of(s, True)

    for ch in range(chunks):
        span = slice(ch * m, (ch + 1) * m)
        placed = jnp.zeros((m, part), F32)
        for r in range(n_row):
            placed = placed + jnp.dot(puts[r][span, :], income[r], preferred_element_type=F32)
        hidden[ch, me_c] = (placed + start[span, :]).astype(BF16)
        send_all(ch)
    for s in range(LEAD1):
        first_relay(jnp.int32(s), True)
    for s in range(LEAD2):
        second_relay(jnp.int32(s), True)

    def step(s, carry):
        l = s // chunks
        ch = s % chunks
        relay(s + LEAD2, second_relay)
        relay(s + LEAD1, first_relay)

        @pl.when(ch == 0)
        def _():
            weight_copy(l).wait()

        await_rest(s)
        total = jnp.zeros((m, part), F32)
        for c in range(n_col):
            values = hidden[s, c].astype(F32)
            total = total + values * values
        mean = jnp.sum(total, axis=1, keepdims=True) * (1.0 / width)
        inverse = lax.rsqrt(mean + epsilon)
        for c in range(n_col):
            cols = slice(c * part, (c + 1) * part)
            values = hidden[s, c].astype(F32) * inverse * gain[l, :, cols]
            half = 0.5 * values
            active[:, cols] = (half + half * jnp.tanh(half)).astype(BF16)
        update = jnp.dot(active[...], weight[l], preferred_element_type=F32)
        result = (hidden[s, me_c].astype(F32) + update).astype(BF16)

        drain_own(s)

        @pl.when(l < layers - 1)
        def _():
            hidden[s + chunks, me_c] = result
            send_all(s + chunks)

        @pl.when(l == layers - 1)
        def _():
            out_ref[ch] = result

        return carry

    lax.fori_loop(0, steps, step, 0)

    for ch in range(chunks):
        first_relay(jnp.int32(steps - chunks + ch), False)
        second_relay(jnp.int32(steps - chunks + ch), False)
    for j in range(1, n_row):
        id_row_copy(j).wait_send()
        row_copy(j).wait_send()
    for j in range(1, n_col):
        piece_copy(j).wait_send()
        id_col_copy(j).wait_send()


def shards(rows, task_ids, task_embed, norm_gain, layer_weight):
    rows_dev, width = rows.shape
    tasks = task_embed.shape[0]
    layers = layer_weight.shape[0]
    part = layer_weight.shape[2]
    n_row = lax.axis_size("row")
    n_col = lax.axis_size("col")
    slots = rows_dev * n_col
    cap = -(-(slots // n_row + tasks) // 16) * 16
    chunks = CHUNKS
    m = slots // chunks
    lead_dim = -(-n_row // 8) * 8
    sizes = (n_row, n_col, layers, chunks, tasks, cap)
    dma = pltpu.SemaphoreType.DMA
    vmem = pl.BlockSpec(memory_space=pltpu.VMEM)
    out = pl.pallas_call(
        functools.partial(kernel, sizes),
        out_shape=jax.ShapeDtypeStruct((chunks, m, part), BF16),
        in_specs=[vmem, vmem, vmem, vmem, pl.BlockSpec(memory_space=pl.ANY)],
        out_specs=vmem,
        scratch_shapes=[
            pltpu.VMEM((layers, width, part), BF16),
            pltpu.VMEM((layers * chunks, n_col, m, part), BF16),
            pltpu.VMEM((m, width), BF16),
            pltpu.VMEM((layers, 1, width), F32),
            pltpu.VMEM((n_col, rows_dev, part), BF16),
            pltpu.VMEM((n_row, cap, part), BF16),
            pltpu.VMEM((n_row, cap, part), BF16),
            pltpu.VMEM((lead_dim, slots), jnp.int32),
            pltpu.VMEM((n_row, lead_dim, slots), jnp.int32),
            pltpu.VMEM((lead_dim, slots), jnp.int32),
            pltpu.VMEM((n_col, lead_dim, slots), jnp.int32),
            dma((layers,)),
            dma((n_col,)),
            dma((n_col,)),
            dma((n_row,)),
            dma((n_row,)),
            dma((n_col,)),
            dma((n_col,)),
            dma((n_row,)),
            dma((n_row,)),
            dma((chunks, n_col)),
            dma((chunks, n_col)),
            dma((chunks, n_col // INNER, max(1, n_col // INNER // 2))),
            dma((layers * chunks, n_col)),
        ],
        compiler_params=pltpu.CompilerParams(
            collective_id=0, has_side_effects=True, vmem_limit_bytes=60 * 1024 * 1024
        ),
    )(rows, task_ids.reshape(1, rows_dev), task_embed, norm_gain, layer_weight)
    return out.reshape(slots, part)


def solution(mesh):
    return jax.shard_map(
        shards,
        mesh=mesh,
        in_specs=(P(("row", "col"), None), P(("row", "col")), P(), P(), P(None, None, "col")),
        out_specs=P("row", "col"),
        check_vma=False,
    )
```
